64 devices in a mesh: rep: 4 (over x, y), dp: 16 (over z, core).
Axes of the slice: x: 2, y: 2, z: 8, core: 2. Of those that a mesh axis runs over, the one named last changes fastest.
The devices are a block of a 4x4x8 slice.
Arguments:
- x: bfloat16 [64, 2048, 512], P(('rep', 'dp')), parts along dimension 0
- dy: bfloat16 [64, 2048, 512], P(('rep', 'dp')), parts along dimension 0
- w_gate: bfloat16 [2, 512, 1280], replicated
- w_up: bfloat16 [2, 512, 1280], replicated
- w_down: bfloat16 [2, 1280, 512], replicated
- m_w_gate: float32 [2, 512, 1280], P(None, 'dp')
- m_w_up: float32 [2, 512, 1280], P(None, 'dp')
- m_w_down: float32 [2, 1280, 512], P(None, 'dp')
- v_w_gate: float32 [2, 512, 1280], P(None, 'dp')
- v_w_up: float32 [2, 512, 1280], P(None, 'dp')
- v_w_down: float32 [2, 1280, 512], P(None, 'dp')
Outputs:
- output 1: bfloat16 [8, 512, 1280], P('rep'), parts along dimension 0
- output 2: bfloat16 [8, 512, 1280], P('rep'), parts along dimension 0
- output 3: bfloat16 [8, 1280, 512], P('rep'), parts along dimension 0
- output 4: float32 [8, 512, 1280], P('rep', 'dp'), parts along dimension 0
- output 5: float32 [8, 512, 1280], P('rep', 'dp'), parts along dimension 0
- output 6: float32 [8, 1280, 512], P('rep', 'dp'), parts along dimension 0
- output 7: float32 [8, 512, 1280], P('rep', 'dp'), parts along dimension 0
- output 8: float32 [8, 512, 1280], P('rep', 'dp'), parts along dimension 0
- output 9: float32 [8, 1280, 512], P('rep', 'dp'), parts along dimension 0
There are 4 independent parts. The reference program is written for one: setup_inputs(seed, part) draws one part's arguments, and reference() takes and returns one part's arrays. A program takes and returns all parts, laid end to end along the dimension named above; an argument that names none is the same for every part.
All inputs are finite; a program needn't handle non-finite values.
Results may differ from the reference program's by a relative error of at most 0.022.
Values are sent between devices in bfloat16 or wider.
A program may use at most 768 MiB of HBM per device.

```python
import jax
import jax.numpy as jnp
from jax import lax

SEQUENCES = 16
TOKENS = 2048
D = 512
FF = 1280
LAYERS = 2
NAMES = ("w_gate", "w_up", "w_down")
SHAPES = {"w_gate": (LAYERS, D, FF), "w_up": (LAYERS, D, FF), "w_down": (LAYERS, FF, D)}


def bump(key, n, height):
    away = (jnp.arange(n, dtype=jnp.int32) - jax.random.randint(key, (), 0, n, jnp.int32)) % n
    return jnp.where(away < n // 8, height, 1.0)


def together(key, own, strength):
    shared = jax.random.normal(key, own.shape[1:], jnp.float32)
    return (own + strength * shared) * lax.rsqrt(1 + strength * strength)


def setup_inputs(seed: int = 0, part: int = 0) -> dict:
    kx, kdy, ka, kb, kz, kf, kh, kl, *keys = jax.random.split(jax.random.key(seed), 8 + 3 * len(NAMES))
    kx, kdy, ka, kb = (jax.random.fold_in(k, part) for k in (kx, kdy, ka, kb))
    kw, km, kv = (keys[i::3] for i in range(3))
    shape = (SEQUENCES, TOKENS, D)
    much_x, much_dy = jax.random.uniform(kz, (2,), jnp.float32, 0.0, 1.0)
    loud = 2.0 ** jax.random.uniform(jax.random.fold_in(kz, 1), (), jnp.float32, -1.0, 2.0)
    layers = 2.0 ** jax.random.uniform(kl, (LAYERS, 1, 1), jnp.float32, -1.0, 1.0)
    x = together(ka, jax.random.normal(kx, shape, jnp.float32), much_x) * bump(kf, D, 4.0)
    dy = together(kb, jax.random.normal(kdy, shape, jnp.float32), much_dy)
    drawn = {"x": x.astype(jnp.bfloat16), "dy": (loud * dy * (SEQUENCES * TOKENS) ** -0.5).astype(jnp.bfloat16)}
    for key, name in zip(kw, NAMES, strict=True):
        w = jax.random.normal(key, SHAPES[name], jnp.float32) * SHAPES[name][1] ** -0.5
        drawn[name] = (w * {"w_gate": 1.0, "w_up": bump(kh, FF, 4.0), "w_down": layers}[name]).astype(jnp.bfloat16)
    for key, name in zip(km, NAMES, strict=True):
        drawn[f"m_{name}"] = 0.1 * jax.random.normal(key, SHAPES[name], jnp.float32)
    for key, name in zip(kv, NAMES, strict=True):
        drawn[f"v_{name}"] = jax.random.uniform(key, SHAPES[name], jnp.float32, 0.005, 0.015)
    return drawn


def matmul(a, w):
    return jnp.dot(a, w, preferred_element_type=jnp.float32).astype(jnp.bfloat16)


def normed(h):
    wide = h.astype(jnp.float32)
    scale = lax.rsqrt(jnp.mean(wide**2, -1, keepdims=True) + 1e-6)
    return (wide * scale).astype(jnp.bfloat16)


def layer(h, w):
    a = normed(h)
    gate = jnp.dot(a, w["w_gate"], preferred_element_type=jnp.float32)
    up = jnp.dot(a, w["w_up"], preferred_element_type=jnp.float32)
    return h + matmul((jax.nn.silu(gate) * up).astype(jnp.bfloat16), w["w_down"])


def adamw(w, m, v, g):
    m = 0.9 * m + 0.1 * g
    v = 0.95 * v + 0.05 * g * g
    step = m * lax.rsqrt(v + 1e-8) + 0.1 * w
    return (w - 0.02 * step).astype(jnp.bfloat16), m, v


def clipped(gradients, sum_of_squares, count):
    factor = jnp.minimum(1.0, 0.5 * lax.rsqrt(sum_of_squares / count + 1e-30))
    return [g * factor for g in gradients]


def stack(weights, h):
    return lax.scan(lambda h, w: (layer(h, w), None), h, weights)[0]


def reference(x, dy, w_gate, w_up, w_down, m_w_gate, m_w_up, m_w_down, v_w_gate, v_w_up, v_w_down):
    weights = dict(zip(NAMES, (w_gate, w_up, w_down), strict=True))

    def take(so_far, sequence):
        h, by_y = sequence
        _, back = jax.vjp(lambda w: stack(w, h), weights)
        return jax.tree.map(lambda total, term: total + term.astype(jnp.float32), so_far, back(by_y)[0]), None

    none_yet = {name: jnp.zeros(w.shape, jnp.float32) for name, w in weights.items()}
    by_weights, _ = lax.scan(take, none_yet, (x, dy))
    gradients = [by_weights[name].astype(jnp.bfloat16).astype(jnp.float32) for name in NAMES]
    gradients = clipped(gradients, sum(jnp.sum(g * g) for g in gradients), sum(g.size for g in gradients))
    new = [
        adamw(w.astype(jnp.float32), m, v, g)
        for w, m, v, g in zip((w_gate, w_up, w_down), (m_w_gate, m_w_up, m_w_down), (v_w_gate, v_w_up, v_w_down), gradients, strict=True)
    ]
    return tuple(one[which] for which in range(3) for one in new)
```

```python
import functools

import jax
import jax.numpy as jnp
from jax import lax
from jax.experimental import pallas as pl
from jax.experimental.pallas import tpu as pltpu
from jax.sharding import PartitionSpec as P

MESH = pl.DeviceIdType.MESH
F32, BF16 = jnp.float32, jnp.bfloat16


def dot(a, b, ca, cb):
    return lax.dot_general(a, b, (((ca,), (cb,)), ((), ())), preferred_element_type=F32)


def scale_of(wide):
    return lax.rsqrt(jnp.mean(wide * wide, -1, keepdims=True) + 1e-6)


def normed(h):
    wide = h.astype(F32)
    return (wide * scale_of(wide)).astype(BF16)


def sigmoid(t):
    return 0.5 * jnp.tanh(0.5 * t) + 0.5


def rounded(t):
    return t.astype(BF16).astype(F32)


def kernel(n, tile, *refs):
    ins, outs, rest = refs[:11], refs[11:22], refs[22:]
    x_in, dy_in, *w_in = ins[:5]
    m_in, v_in = ins[5:8], ins[8:11]
    w_out, m_out, v_out = outs[0:3], outs[3:6], outs[6:9]
    kept_gate, kept_up = outs[9:11]
    h_ref, dh_ref, a_refs, w_refs = rest[0], rest[1], rest[2:4], rest[4:7]
    u_ref, dg_ref, du_ref, gate_ref, up_ref = rest[7:12]
    m_refs, v_refs = rest[12:15], rest[15:18]
    kinds = {"wide": rest[18:24], "tall": rest[24:30]}
    norms = rest[30]
    (load_sem, keep_sem, swap_s, swap_r, ring_s, ring_r, norm_s, norm_r, own_s, state_s, ag_s, ag_r, mate_s, mate_r, out_s) = rest[31:]

    tokens, d = h_ref.shape
    ff = u_ref.shape[1]
    half_way = n // 4
    me = lax.axis_index("dp")
    chip, core = me // 2, lax.rem(me, 2)
    chips = n // 2
    mate = me + 1 - 2 * core
    ahead = (lax.rem(me + 2, n), lax.rem(me + n - 2, n))

    def remote(src, dst, send, recv, to):
        return pltpu.make_async_remote_copy(
            src_ref=src, dst_ref=dst, send_sem=send, recv_sem=recv, device_id={"dp": to}, device_id_type=MESH
        )

    barrier = pltpu.get_barrier_semaphore()
    for k in range(1, n):
        pl.semaphore_signal(barrier, inc=1, device_id={"dp": lax.rem(me + k, n)}, device_id_type=MESH)

    loads = []

    def load(src, dst):
        copy = pltpu.make_async_copy(src, dst, load_sem.at[len(loads)])
        copy.start()
        loads.append(copy)
        return copy

    for src, dst in ((x_in.at[0], h_ref), (w_in[0].at[0], w_refs[0].at[0]), (w_in[1].at[0], w_refs[1].at[0]), (w_in[2].at[0], w_refs[2].at[0])):
        load(src, dst)
    for which in range(3):
        load(w_in[which].at[1], w_refs[which].at[1])
    load(dy_in.at[0], dh_ref)
    n_first = len(loads)
    for which in range(3):
        load(m_in[which], m_refs[which])
        load(v_in[which], v_refs[which])
    for copy in loads[:n_first]:
        copy.wait()

    wg, wu, wd = w_refs
    cuts = (slice(0, 2 * ff // 5), slice(2 * ff // 5, ff))

    def keep(rows):
        return (
            pltpu.make_async_copy(gate_ref, kept_gate.at[rows, :], keep_sem.at[0]),
            pltpu.make_async_copy(up_ref, kept_up.at[rows, :], keep_sem.at[1]),
        )

    def rows_of(t, size):
        return pl.ds(pl.multiple_of(t * size, size), size)

    def forward(t, _):
        rows = rows_of(t, tile)

        @pl.when(t > 0)
        def _():
            for copy in keep(rows_of(t - 1, tile)):
                copy.wait()

        x = h_ref[rows, :]
        a = normed(x)
        a_refs[0][rows, :] = a
        for cut in cuts:
            gate, up = dot(a, wg[0, :, cut], 1, 0), dot(a, wu[0, :, cut], 1, 0)
            gate_ref[:, cut] = gate
            up_ref[:, cut] = up
            u_ref[rows, cut] = (gate * sigmoid(gate) * up).astype(BF16)
        for copy in keep(rows):
            copy.start()
        h = (x.astype(F32) + rounded(dot(u_ref[rows, :], wd[0], 1, 0))).astype(BF16)
        h_ref[rows, :] = h
        a = normed(h)
        a_refs[1][rows, :] = a
        by_y = dh_ref[rows, :]
        for cut in cuts:
            gate, up = dot(a, wg[1, :, cut], 1, 0), dot(a, wu[1, :, cut], 1, 0)
            through(rows, cut, gate, up, rounded(dot(by_y, wd[1, cut, :], 1, 1)))
        return 0

    def through(rows, cut, gate, up, by_u):
        sig = sigmoid(gate)
        silu = gate * sig
        u_ref[rows, cut] = (silu * up).astype(BF16)
        du_ref[rows, cut] = (by_u * silu).astype(BF16)
        dg_ref[rows, cut] = (by_u * up * (sig + silu * (1.0 - sig))).astype(BF16)

    tiles = tokens // tile
    lax.fori_loop(0, tiles, forward, 0)
    for copy in keep(rows_of(tiles - 1, tile)):
        copy.wait()

    part = tile // 2

    def bring(t, side):
        rows = pl.ds(pl.multiple_of(t * tile + side * part, part), part)
        here = pl.ds(side * part, part)
        return (
            pltpu.make_async_copy(kept_gate.at[rows, :], gate_ref.at[here, :], keep_sem.at[2 + side]),
            pltpu.make_async_copy(kept_up.at[rows, :], up_ref.at[here, :], keep_sem.at[4 + side]),
        )

    for side in range(2):
        for copy in bring(0, side):
            copy.start()

    def into_norm(t, _):
        rows = rows_of(t, tile)
        by_a = rounded(rounded(dot(dg_ref[rows, :], wg[1], 1, 1)) + rounded(dot(du_ref[rows, :], wu[1], 1, 1)))
        wide = h_ref[rows, :].astype(F32)
        scale = scale_of(wide)
        unit = wide * scale
        by_h = scale * (by_a - unit * jnp.mean(by_a * unit, -1, keepdims=True))
        dh_ref[rows, :] = (dh_ref[rows, :].astype(F32) + rounded(by_h)).astype(BF16)
        return 0

    def into_hidden(t, _):
        by_u = rounded(dot(dh_ref[rows_of(t, tile), :], wd[0], 1, 1))
        for side in range(2):
            for copy in bring(t, side):
                copy.wait()
            here = slice(side * part, (side + 1) * part)
            rows = pl.ds(pl.multiple_of(t * tile + side * part, part), part)
            through(rows, slice(None), gate_ref[here, :], up_ref[here, :], by_u[here])

        @pl.when(t + 1 < tiles)
        def _():
            for side in range(2):
                for copy in bring(t + 1, side):
                    copy.start()

        return 0

    sent = []
    pending = {}

    def of(kind, slot):
        total, _, back, ring, first, result = kinds[kind]
        return total.at[slot], None, back.at[slot], ring.at[slot], first.at[slot], result.at[slot]

    def swap(number, kind, slot, left, right, cuts):
        total, _, back, *_ = of(kind, slot)
        out = kinds[kind][1].at[slot // 2 if kind == "wide" else 0]
        rows = total.shape[1]
        if number >= 3:
            pending[number - 3][2].wait_send()
        for first, last in zip(cuts[:-1], cuts[1:], strict=True):
            pairs = dot(left[...], right[:, first:last], 0, 0).reshape(chips, 2, rows, last - first)
            low, high = pairs[:, 0], pairs[:, 1]
            total[:, :, first:last] = jnp.where(core == 0, low, high)
            out[:, :, first:last] = jnp.where(core == 0, high, low).astype(BF16)
        copy = remote(out, back, swap_s.at[number], swap_r.at[number], mate)
        copy.start()
        if number >= 3:
            sent.append(copy)
        pending[number] = (kind, slot, copy)

    def halves(columns):
        return slice(0, columns // 2), slice(columns // 2, columns)

    def hop(number, way, step, src, dst):
        return remote(src, dst, ring_s.at[number, way, step], ring_r.at[number, way, step], ahead[way])

    def block_at(step, way):
        return lax.rem(chip + half_way - 1 - step + chips, chips) if way == 0 else lax.rem(chip - half_way + 1 + step + chips, chips)

    def arriving(number, way, step, kind, slot):
        _, _, _, ring, first, _ = of(kind, slot)
        columns = ring.shape[3]
        if step:
            return hop(number, way, step, ring.at[way, step - 1], ring.at[way, step])
        side = pl.ds(0, columns // 2) if way == 0 else pl.ds(columns // 2, columns // 2)
        return hop(number, way, 0, first.at[way], ring.at[way, 0, :, side])

    def send(number, step, kind, slot):
        for way in range(2):
            copy = arriving(number, way, step, kind, slot)
            copy.start()
            sent.append(copy)

    def advance(number, stage):
        kind, slot, copy = pending[number]
        total, _, back, ring, first, result = of(kind, slot)
        sides = halves(total.shape[2])
        if stage == 0:
            copy.wait_recv()
            total[...] += back[...].astype(F32)
            far = total[lax.rem(chip + half_way, chips)]
            for way in range(2):
                first[way] = far[:, sides[way]].astype(BF16)
            send(number, 0, kind, slot)
            return
        for way in range(2):
            arriving(number, way, stage - 1, kind, slot).wait_recv()
            if stage < half_way:
                own = total[block_at(stage - 1, way)]
                if stage == 1:
                    ring[way, 0, :, sides[way]] = (own[:, sides[way]] + ring[way, 0, :, sides[way]].astype(F32)).astype(BF16)
                    ring[way, 0, :, sides[1 - way]] = own[:, sides[1 - way]].astype(BF16)
                else:
                    ring[way, stage - 1] = (own + ring[way, stage - 1].astype(F32)).astype(BF16)
        if stage < half_way:
            send(number, stage, kind, slot)
            return
        grad = rounded(total[chip] + ring[0, half_way - 1].astype(F32) + ring[1, half_way - 1].astype(F32))
        result[...] = grad
        squares = jnp.sum((grad * grad).reshape(-1, 8, grad.shape[1]), 0)
        squares = sum(squares[:, i : i + 128] for i in range(0, squares.shape[1], 128))
        norms[me] = squares if number == 0 else norms[me] + squares

    def by_down(number, slot):
        swap(number, "tall", slot, u_ref, dh_ref, (0, d // 2, d))

    def by_wide(number, slot, a, hidden):
        swap(number, "wide", slot, a, hidden, (0, 3 * ff // 5, ff))

    pl.semaphore_wait(barrier, n - 1)
    by_down(0, 1)
    by_wide(1, 1, a_refs[1], dg_ref)
    advance(0, 0)
    by_wide(2, 3, a_refs[1], du_ref)
    advance(0, 1)
    advance(1, 0)
    lax.fori_loop(0, tiles // 2, into_norm, 0)
    advance(0, 2)
    advance(1, 1)
    advance(2, 0)
    lax.fori_loop(tiles // 2, tiles, into_norm, 0)
    advance(0, 3)
    advance(1, 2)
    advance(2, 1)
    lax.fori_loop(0, tiles // 2, into_hidden, 0)
    advance(0, 4)
    advance(1, 3)
    advance(2, 2)
    lax.fori_loop(tiles // 2, tiles, into_hidden, 0)
    by_down(3, 0)
    advance(1, 4)
    advance(2, 3)
    by_wide(4, 0, a_refs[0], dg_ref)
    advance(3, 0)
    advance(2, 4)
    by_wide(5, 2, a_refs[0], du_ref)
    for now in range(7):
        for number in (3, 4, 5):
            stage = now + 4 - number
            if (number, stage) != (3, 0) and 0 <= stage <= half_way:
                advance(number, stage)

    count = sum(w.size for w in w_refs)
    for k in range(1, n):
        copy = remote(norms.at[me], norms.at[me], norm_s.at[k], norm_r.at[k], lax.rem(me + k, n))
        copy.start()
        sent.append(copy)
    for copy in loads[n_first:]:
        copy.wait()
    for k in range(1, n):
        other = lax.rem(me + n - k, n)
        remote(norms.at[other], norms.at[other], norm_s.at[k], norm_r.at[k], other).wait_recv()
    squares = jnp.sum(jnp.sum(jnp.sum(norms[...], 0), 1, keepdims=True), 0, keepdims=True)
    factor = jnp.minimum(1.0, 0.5 * lax.rsqrt(squares / count + 1e-30))

    local = []

    def start(copy, to):
        copy.start()
        to.append(copy)

    def piece(ref, which, layer, device, side=None):
        rows = ref.shape[1] // n
        at = ref.at[layer, pl.ds(pl.multiple_of(device * rows, rows), rows)]
        if side is None:
            return at
        columns = ref.shape[2] // 2
        return ref.at[layer, pl.ds(pl.multiple_of(device * rows, rows), rows), pl.ds(side * columns, columns)]

    order = [(layer, which) for layer in (1, 0) for which in (2, 0, 1)]
    slots = {(1, 2): ("tall", 1), (1, 0): ("wide", 1), (1, 1): ("wide", 3), (0, 2): ("tall", 0), (0, 0): ("wide", 0), (0, 1): ("wide", 2)}

    def to_mate(i, layer, which, place, device, side=None):
        return remote(
            piece(w_refs[which], which, layer, device, side), piece(w_out[which], which, layer, device, side),
            mate_s.at[i, place], mate_r.at[i, place], mate,
        )

    def to_out(i, layer, which, place, device, side=None):
        return pltpu.make_async_copy(
            piece(w_refs[which], which, layer, device, side), piece(w_out[which], which, layer, device, side), out_s.at[i, place]
        )

    def along(i, layer, which, way, step, device, side=None):
        at = piece(w_refs[which], which, layer, device, side)
        return remote(at, at, ag_s.at[i, way, step], ag_r.at[i, way, step], ahead[way])

    for i, (layer, which) in enumerate(order):
        kind, slot = slots[layer, which]
        g = of(kind, slot)[5][...] * factor
        m = 0.9 * m_refs[which][layer] + 0.1 * g
        v = 0.95 * v_refs[which][layer] + 0.05 * g * g
        m_refs[which][layer] = m
        v_refs[which][layer] = v
        rows = w_refs[which].shape[1] // n
        mine = pl.ds(pl.multiple_of(me * rows, rows), rows)
        w = w_refs[which][layer, mine, :].astype(F32)
        w_refs[which][layer, mine, :] = (w - 0.02 * (m * lax.rsqrt(v + 1e-8) + 0.1 * w)).astype(BF16)
        for way in range(2):
            start(along(i, layer, which, way, 0, me), sent)
        start(to_mate(i, layer, which, 0, me), sent)
        start(to_out(i, layer, which, 0, me), local)
        start(pltpu.make_async_copy(m_refs[which].at[layer], m_out[which].at[layer], state_s.at[0, i]), local)
        start(pltpu.make_async_copy(v_refs[which].at[layer], v_out[which].at[layer], state_s.at[1, i]), local)

    def origin(way, hops):
        return lax.rem(me + 2 * (n - hops), n) if way == 0 else lax.rem(me + 2 * hops, n)

    for hops in range(1, half_way + 1):
        for i, (layer, which) in enumerate(order):
            for way in range(2):
                device = origin(way, hops)
                side = way if hops == half_way else None
                along(i, layer, which, way, hops - 1, device, side).wait_recv()
                if hops < half_way:
                    start(along(i, layer, which, way, hops, device, way if hops == half_way - 1 else None), sent)
                place = 2 * hops - 1 + way
                start(to_mate(i, layer, which, place, device, side), sent)
                start(to_out(i, layer, which, place, device, side), local)

    for i, (layer, which) in enumerate(order):
        to_mate(i, layer, which, 0, mate).wait_recv()
        for hops in range(1, half_way + 1):
            for way in range(2):
                device = lax.rem(mate + 2 * (n - hops), n) if way == 0 else lax.rem(mate + 2 * hops, n)
                to_mate(i, layer, which, 2 * hops - 1 + way, device, way if hops == half_way else None).wait_recv()
    for copy in local:
        copy.wait()
    for copy in sent:
        copy.wait_send()


def solution(mesh):
    n = mesh.shape["dp"]

    def step(*args):
        x, w_gate, w_down = args[0], args[2], args[4]
        _, tokens, d = x.shape
        layers, _, ff = w_gate.shape
        chips, way = n // 2, n // 4
        tile = tokens // 4
        weights, moments = args[2:5], args[5:11]
        vmem, dma = pltpu.VMEM, pltpu.SemaphoreType.DMA

        def ring_buffers(slots, rows, columns):
            return [
                vmem((slots, chips, rows, columns), F32),
                vmem((slots // layers, chips, rows, columns), BF16),
                vmem((slots, chips, rows, columns), BF16),
                vmem((slots, 2, way, rows, columns), BF16),
                vmem((slots, 2, rows, columns // 2), BF16),
                vmem((slots, rows, columns), F32),
            ]

        scratch = [
            *(vmem((tokens, d), BF16) for _ in range(4)),
            *(vmem(w.shape, BF16) for w in weights),
            *(vmem((tokens, ff), BF16) for _ in range(3)),
            *(vmem((tile, ff), F32) for _ in range(2)),
            *(vmem(t.shape, F32) for t in moments),
            *ring_buffers(2 * layers, d // n, ff),
            *ring_buffers(layers, ff // n, d),
            vmem((n, 8, 128), F32),
            dma((14,)), dma((6,)), dma((6,)), dma((6,)), dma((6, 2, way)), dma((6, 2, way)), dma((n,)), dma((n,)),
            dma((6,)), dma((2, 6)), dma((6, 2, way)), dma((6, 2, way)), dma((6, 2 * way + 1)), dma((6, 2 * way + 1)), dma((6, 2 * way + 1)),
        ]
        shapes = [jax.ShapeDtypeStruct(w.shape, BF16) for w in weights] + [jax.ShapeDtypeStruct(t.shape, F32) for t in moments]
        shapes += [jax.ShapeDtypeStruct((tokens, ff), F32)] * 2
        anywhere = pl.BlockSpec(memory_space=pl.ANY)
        out = pl.pallas_call(
            functools.partial(kernel, n, tile),
            out_shape=shapes,
            in_specs=[anywhere] * len(args),
            out_specs=[anywhere] * len(shapes),
            scratch_shapes=scratch,
            compiler_params=pltpu.CompilerParams(collective_id=0, has_side_effects=True, vmem_limit_bytes=67_043_328),
            name="train_step",
        )(*args)
        return tuple(out[:9])

    whole, rows = P(None, None, None), P(None, "dp", None)
    return jax.shard_map(
        step,
        mesh=mesh,
        in_specs=(P(("rep", "dp"), None, None),) * 2 + (whole,) * 3 + (rows,) * 6,
        out_specs=(P("rep", None, None),) * 3 + (P("rep", "dp", None),) * 6,
        check_vma=False,
    )
```
